32 devices in a mesh: dp: 8 (over z, y), ep: 4 (over x, core).
Axes of the slice: x: 2, y: 2, z: 4, core: 2. Of those that a mesh axis runs over, the one named last changes fastest.
Arguments:
- tokens: bfloat16 [128, 4096], P(('dp', 'ep')), may hold values from -6 to 6
- router: float32 [4096, 8], replicated, may hold values from -0.1875 to 0.1875
- expert_ids: int32 [128, 2], P(('dp', 'ep')), may hold values from 0 to 7, all different within a row; in each aligned block of 4 rows (0 to 3, 4 to 7, ...) at most 2 rows name the same one
- w_gate: bfloat16 [8, 4096, 12288], P('dp', None, 'ep'), may hold values from -0.09375 to 0.09375
- w_up: bfloat16 [8, 4096, 12288], P('dp', None, 'ep'), may hold values from -0.09375 to 0.09375
- w_down: bfloat16 [8, 12288, 4096], P('dp', 'ep'), may hold values from -0.0546875 to 0.0546875
- states: bfloat16 [128, 16, 8192], P('dp', None, 'ep'), may hold values from -6 to 6
- kv_blocks: bfloat16 [256, 2, 16, 1024], P('dp', None, None, 'ep'), may hold values from -6 to 6
- plan_slots: int32 [8, 2, 3], replicated, may hold values from -1 to 15, as said below
- plan_len: int32 [8, 2], replicated, may hold values from 0 to 32, as said below
- plan_blocks: int32 [8, 2, 2, 2], replicated, may hold values from -1 to 31, as said below
Outputs:
- mixed: bfloat16 [128, 4096], P(('dp', 'ep'))
- new_states: bfloat16 [128, 16, 8192], P('dp', None, 'ep')
- new_cache: bfloat16 [256, 2, 16, 1024], P('dp', None, None, 'ep')
The draws below stay inside these ranges and needn't reach their ends.
Inputs may be any that keep to these rules, and one draw needn't show every extreme that they name: `expert_ids`: in the rows of one device no expert is named more than 2 times. `plan_slots`: A move is live exactly where its first entry is not -1, and then all three entries are set; otherwise all are -1. For each m there is one distance d_m from 1 to 7, distinct for distinct m, such that every live move (r, m) goes to rank (r + d_m) mod 8. The leaving slots of a rank are distinct, the slots taken at a rank are distinct and differ from its leaving slots. Some rank has all 2 moves live. `plan_len`: zero exactly where the move is not live; some move holds 32 tokens. `plan_blocks`: entry j of both tables is -1 exactly where j * 16 >= plan_len. The blocks leaving a rank are distinct, the blocks taken at a rank are distinct and differ from the ones leaving it.
All inputs are finite; a program needn't handle non-finite values.
Results may differ from the reference program's by a relative error of at most 0.005.
Values may be sent and summed in bfloat16 or wider, within the bound.
A program may use at most 128 MiB of HBM per device.

```python
import math
import jax
import jax.numpy as jnp
import numpy as np
from jax import lax

D = 4096
FF = 12288
EXPERTS = 8
CHANNELS = 8192
NST = 16
KVH = 8
HEAD = 128
BLK = 16
TOK_DEV = 4
SLOTS = 16
BLOCKS = 32
MOVE = 2
BPR = 2
CAP = 2
GROUP = 1
TOKENS = 128
N_DP = 8
N_EP = 4


def plan_core(key):
    base = jax.random.fold_in(key, 4242)
    keys = jax.random.split(base, 7)
    offsets = 1 + jax.random.permutation(keys[1], N_DP - 1)[:MOVE]
    rank_line = jnp.arange(N_DP, dtype=jnp.int32)
    target_rank = ((rank_line[:, None] + offsets[None, :]) % N_DP).astype(jnp.int32)
    move_line = jnp.arange(MOVE, dtype=jnp.int32)
    live = jax.random.randint(keys[2], (N_DP, MOVE), 0, 5) < 3
    busiest = jax.random.randint(keys[3], (), 0, N_DP)
    live = live | (rank_line[:, None] == busiest)
    slot_perm = jax.vmap(lambda inner: jax.random.permutation(inner, SLOTS))(jax.random.split(keys[4], N_DP))
    block_perm = jax.vmap(lambda inner: jax.random.permutation(inner, BLOCKS))(jax.random.split(keys[5], N_DP))
    length = jax.random.randint(keys[6], (N_DP, MOVE), 1, BPR * BLK + 1)
    longest = (rank_line[:, None] == busiest) & (move_line[None, :] == 0)
    length = jnp.where(longest, BPR * BLK, length)
    length = jnp.where(live, length, 0).astype(jnp.int32)
    leaving_slot = jnp.where(live, slot_perm[:, :MOVE], -1)
    taken_slot = jnp.where(live, slot_perm[target_rank, MOVE + move_line[None, :]], -1)
    drawn_rank = jnp.where(live, target_rank, -1)
    plan_slots = jnp.stack([leaving_slot, drawn_rank, taken_slot], axis=-1).astype(jnp.int32)
    block_count = (length + BLK - 1) // BLK
    block_line = jnp.arange(BPR, dtype=jnp.int32)
    used = block_line[None, None, :] < block_count[:, :, None]
    leaving_block = block_perm[:, :MOVE * BPR].reshape(N_DP, MOVE, BPR)
    taken_block = block_perm[target_rank[:, :, None], MOVE * BPR + move_line[None, :, None] * BPR + block_line[None, None, :]]
    leaving_block = jnp.where(used, leaving_block, -1)
    taken_block = jnp.where(used, taken_block, -1)
    plan_blocks = jnp.stack([leaving_block, taken_block], axis=2).astype(jnp.int32)
    return (plan_slots, length, plan_blocks)


def draw_plan_slots(key, part):
    return plan_core(key)[0]


def draw_plan_len(key, part):
    return plan_core(key)[1]


def draw_plan_blocks(key, part):
    return plan_core(key)[2]


def levels(own_key, dims, shards, smallest, high):
    factor_of = 1.0
    for axis_at, shards_of in shards:
        draws = jax.random.uniform(jax.random.fold_in(jax.random.fold_in(own_key, 6), axis_at), (shards_of,), jnp.float32, smallest / len(shards), high / len(shards))
        factor_of = factor_of * jnp.repeat(jnp.exp(draws), dims[axis_at] // shards_of).reshape((-1,) + (1,) * (len(dims) - 1 - axis_at))
    return factor_of


def shared_out(key, own, number, rows, count, top, reach, skew):
    order = jax.random.permutation(key, count)
    heavy_load, usual = shares(count, rows * top, reach, skew, True), shares(count, rows * top, reach, skew, False)
    places = jnp.arange(count)

    def named(sizes, rotation):
        used = int((sizes > 0).sum())
        fixed = max(1, used // 4)
        passed = fixed + (places - fixed + rotation * (used - fixed)) % max(1, count - fixed)
        return jnp.zeros((count,), jnp.int32).at[order[jnp.where(places < fixed, places, passed)]].set(jnp.asarray(sizes, jnp.int32))

    sizes = jnp.where(number % 4 == 0, named(heavy_load, number // 4), named(usual, number - number // 4 - 1))
    mixed = jax.random.permutation(jax.random.fold_in(own, 3), count)
    giver, taker = mixed[0:count // 2 * 2:2], mixed[1:count // 2 * 2:2]
    margin = jnp.minimum(sizes[giver] - 1, reach - sizes[taker]) // 2
    margin = jnp.where((giver == order[0]) | (taker == order[0]) | (sizes[taker] == 0), 0, jnp.maximum(margin, 0))
    passed = jax.random.randint(jax.random.fold_in(own, 4), (count // 2,), 0, 1 << 20) % (margin + 1)
    sizes = sizes.at[giver].add(-passed).at[taker].add(passed)
    labels = jnp.searchsorted(jnp.cumsum(sizes), jnp.arange(rows * top), side="right").astype(jnp.int32)
    listing = labels.reshape(top, rows).T
    listing = listing[jax.random.permutation(jax.random.fold_in(own, 1), rows)]
    rotation = jax.random.randint(jax.random.fold_in(own, 2), (rows, 1), 0, top)
    return jnp.take_along_axis(listing, (jnp.arange(top)[None, :] + rotation) % top, axis=1)


def shares(number_of, total, reach, skew, full):
    weights = [(1 << 20) // math.isqrt(rank ** skew) + 1 for rank in range(1, number_of + 1)]
    largest = reach if full else min(reach, max(-(-total // number_of), total * weights[0] // sum(weights)))
    least = 1 if total - largest >= number_of - 1 else 0
    holding, rest = [largest] + [least] * (number_of - 1), total - largest - least * (number_of - 1)
    while rest > 0:
        movable = [i for i in range(1, number_of) if holding[i] < largest] or [i for i in range(1, number_of) if holding[i] < reach]
        whole, left = sum([weights[i] for i in movable]), rest
        for i in movable:
            addition = min(reach - holding[i], max(1, left * weights[i] // whole), rest)
            holding[i] = holding[i] + addition
            rest = rest - addition
    return np.array(holding)


def bell_draw(rng, shape, scale, limit, pieces=(), held_as=jnp.bfloat16):
    values = scale * jax.random.normal(rng, shape, jnp.float32)
    if pieces:
        values = values * levels(rng, shape, pieces, -0.22, 0.18)
    return jnp.clip(values, -limit, limit).astype(held_as)


def setup_inputs(seed: int = 0) -> dict:
    streams_of = jax.random.split(jax.random.key(seed), 12)
    tokens = bell_draw(streams_of[0], (TOKENS, D), 1.0, 6.0, ((0, 32),))
    router = bell_draw(streams_of[1], (D, EXPERTS), (D // 4) ** -0.5, 0.1875, (), jnp.float32)
    expert_ids_keys = jax.random.split(jax.random.fold_in(streams_of[2], 1), TOKENS // TOK_DEV)
    expert_ids_turns = jax.random.permutation(jax.random.fold_in(streams_of[2], 3), TOKENS // TOK_DEV)
    expert_ids = jax.vmap(lambda own, number: shared_out(jax.random.fold_in(streams_of[2], 2), own, number, TOK_DEV, EXPERTS, 2, CAP, 2))(expert_ids_keys, expert_ids_turns).reshape((TOKENS, 2))
    w_gate = bell_draw(streams_of[3], (EXPERTS * GROUP, D, FF // GROUP), D ** -0.5, 0.09375, ((0, 8), (2, 4)))
    w_up = bell_draw(streams_of[4], (EXPERTS * GROUP, D, FF // GROUP), D ** -0.5, 0.09375, ((0, 8), (2, 4)))
    w_down = bell_draw(streams_of[5], (EXPERTS * GROUP, FF // GROUP, D), FF ** -0.5, 0.0546875, ((0, 8), (1, 4)))
    states = bell_draw(streams_of[6], (N_DP * SLOTS, NST, CHANNELS), 1.0, 6.0, ((0, 8), (2, 4)))
    kv_blocks = bell_draw(streams_of[7], (N_DP * BLOCKS, 2, BLK, KVH * HEAD), 1.0, 6.0, ((0, 8), (3, 4)))
    plan_slots = draw_plan_slots(jax.random.fold_in(streams_of[11], 71), 0)
    plan_len = draw_plan_len(jax.random.fold_in(streams_of[11], 71), 0)
    plan_blocks = draw_plan_blocks(jax.random.fold_in(streams_of[11], 71), 0)
    return dict(tokens=tokens, router=router, expert_ids=expert_ids, w_gate=w_gate, w_up=w_up, w_down=w_down, states=states, kv_blocks=kv_blocks, plan_slots=plan_slots, plan_len=plan_len, plan_blocks=plan_blocks)


def reference(tokens, router, expert_ids, w_gate, w_up, w_down, states, kv_blocks, plan_slots, plan_len, plan_blocks):
    devices_all = N_DP * N_EP
    block_tokens = tokens.reshape(devices_all, TOK_DEV, D)
    pick_ids = expert_ids.reshape(devices_all, TOK_DEV * 2).astype(jnp.int32)
    onehot = (pick_ids[:, :, None] == jnp.arange(EXPERTS, dtype=jnp.int32)[None, None, :]).astype(jnp.int32)
    earlier = jnp.cumsum(onehot, axis=1) - onehot
    slot_of = jnp.sum(earlier * onehot, axis=2).astype(jnp.int32)
    target_row = (pick_ids * CAP + slot_of).astype(jnp.int32)
    doubled = jnp.repeat(block_tokens, 2, axis=1)
    device_line = jnp.broadcast_to(jnp.arange(devices_all, dtype=jnp.int32)[:, None], target_row.shape)
    packed = jnp.zeros((devices_all, EXPERTS * CAP, D), tokens.dtype)
    packed = packed.at[device_line.reshape(-1), target_row.reshape(-1)].set(doubled.reshape(-1, D))
    expert_rows = packed.reshape(devices_all, EXPERTS, CAP, D).transpose(1, 0, 2, 3).reshape(EXPERTS, devices_all * CAP, D)
    slab_width = FF // GROUP
    gate_all = w_gate.reshape(EXPERTS, GROUP, D, slab_width)
    up_all = w_up.reshape(EXPERTS, GROUP, D, slab_width)
    down_all = w_down.reshape(EXPERTS, GROUP * slab_width, D)

    def run_expert(operands):
        rows, gate_slabs, up_slabs, down_matrix = operands
        gate_matrix = gate_slabs.transpose(1, 0, 2).reshape(D, FF)
        up_matrix = up_slabs.transpose(1, 0, 2).reshape(D, FF)
        gate = jnp.dot(rows, gate_matrix, preferred_element_type=jnp.float32)
        upper = jnp.dot(rows, up_matrix, preferred_element_type=jnp.float32)
        hidden = (jax.nn.silu(gate) * upper).astype(jnp.bfloat16)
        return jnp.dot(hidden, down_matrix, preferred_element_type=jnp.float32)

    expert_out = lax.map(run_expert, (expert_rows, gate_all, up_all, down_all))
    expert_out = expert_out.reshape(EXPERTS, devices_all, CAP, D)
    chosen = expert_out[pick_ids, device_line, slot_of]
    chosen = chosen.reshape(TOKENS, 2, D)
    logits = jnp.dot(tokens.astype(jnp.float32), router, precision=lax.Precision.HIGHEST)
    scores = jax.nn.sigmoid(jnp.take_along_axis(logits, expert_ids.astype(jnp.int32), axis=1))
    weights = scores / jnp.sum(scores, axis=1, keepdims=True)
    mixed = jnp.sum(weights[:, :, None] * chosen, axis=1).astype(jnp.bfloat16)

    rank_line = jnp.arange(N_DP, dtype=jnp.int32)
    slot_states = states.reshape(N_DP, SLOTS, NST, CHANNELS)
    leaving_slot = plan_slots[:, :, 0].astype(jnp.int32)
    target_rank = plan_slots[:, :, 1].astype(jnp.int32)
    target_slot = plan_slots[:, :, 2].astype(jnp.int32)
    gone = jnp.any(leaving_slot[:, :, None] == jnp.arange(SLOTS, dtype=jnp.int32)[None, None, :], axis=1)
    payload = slot_states[rank_line[:, None], jnp.maximum(leaving_slot, 0)]
    payload = jnp.where((leaving_slot >= 0)[:, :, None, None], payload, jnp.zeros_like(payload))
    new_states = jnp.where(gone[:, :, None, None], jnp.zeros_like(slot_states), slot_states)
    rank_index = jnp.where(target_rank >= 0, target_rank, N_DP).astype(jnp.int32)
    slot_index = jnp.maximum(target_slot, 0).astype(jnp.int32)
    new_states = new_states.at[rank_index.reshape(-1), slot_index.reshape(-1)].set(payload.reshape(-1, NST, CHANNELS), mode="drop")
    new_states = new_states.reshape(N_DP * SLOTS, NST, CHANNELS)

    cache = kv_blocks.reshape(N_DP, BLOCKS, 2, BLK, KVH * HEAD)
    leaving_block = plan_blocks[:, :, 0, :].astype(jnp.int32)
    taken_block = plan_blocks[:, :, 1, :].astype(jnp.int32)
    gone_blocks = jnp.any(leaving_block.reshape(N_DP, -1)[:, :, None] == jnp.arange(BLOCKS, dtype=jnp.int32)[None, None, :], axis=1)
    cache_payload = cache[rank_line[:, None, None], jnp.maximum(leaving_block, 0)]
    position = jnp.arange(BPR, dtype=jnp.int32)[:, None] * BLK + jnp.arange(BLK, dtype=jnp.int32)[None, :]
    written = (leaving_block >= 0)[:, :, :, None] & (position[None, None] < plan_len.astype(jnp.int32)[:, :, None, None])
    cache_payload = jnp.where(written[:, :, :, None, :, None], cache_payload, jnp.zeros_like(cache_payload))
    new_cache = jnp.where(gone_blocks[:, :, None, None, None], jnp.zeros_like(cache), cache)
    block_rank = jnp.where(taken_block >= 0, jnp.broadcast_to(target_rank[:, :, None], taken_block.shape), N_DP).astype(jnp.int32)
    block_index = jnp.maximum(taken_block, 0).astype(jnp.int32)
    new_cache = new_cache.at[block_rank.reshape(-1), block_index.reshape(-1)].set(cache_payload.reshape(-1, 2, BLK, KVH * HEAD), mode="drop")
    new_cache = new_cache.reshape(N_DP * BLOCKS, 2, BLK, KVH * HEAD)
    return mixed, new_states, new_cache
```

```python
import functools

import jax
import jax.numpy as jnp
from jax import lax
from jax.experimental import pallas as pl
from jax.experimental.pallas import tpu as pltpu
from jax.sharding import PartitionSpec as P

CAP = 2
MESH = pl.DeviceIdType.MESH
ANY = pl.BlockSpec(memory_space=pl.ANY)
VMEM = pl.BlockSpec(memory_space=pltpu.VMEM)
SMEM = pl.BlockSpec(memory_space=pltpu.SMEM)
VMEM_LIMIT = 67_000_000
UP_TILE = 256
DOWN_TILE = 512
RING = 8


def target_rows(ids_ref, tok_count):
    picks = [ids_ref[t, k] for t in range(tok_count) for k in range(2)]
    rows = []
    for p, expert in enumerate(picks):
        slot = jnp.int32(0)
        for q in range(p):
            slot = slot + jnp.where(picks[q] == expert, 1, 0)
        rows.append(expert * CAP + slot)
    return picks, rows


def prepare_kernel(
    ids_ref, slots_ref, len_ref, blocks_ref, tok_ref, states_ref, kv_ref,
    packed_ref, send_state, send_cache, base_states, base_cache,
    s_buf, c_buf, s_pay, c_pay, load_sem, pay_sem, cpay_sem, store_sem,
):
    here = lax.axis_index("dp")
    moves = slots_ref.shape[1]
    per_request = blocks_ref.shape[3]
    block_len = kv_ref.shape[2]
    load_s = pltpu.make_async_copy(states_ref, s_buf, load_sem.at[0])
    load_c = pltpu.make_async_copy(kv_ref, c_buf, load_sem.at[1])
    load_s.start()
    load_c.start()
    tok_count = tok_ref.shape[0]
    experts = packed_ref.shape[0]
    _, rows = target_rows(ids_ref, tok_count)
    row_at = lax.broadcasted_iota(jnp.int32, (experts * CAP, tok_count), 0)
    tok_at = lax.broadcasted_iota(jnp.int32, (experts * CAP, tok_count), 1)
    placer = jnp.zeros((experts * CAP, tok_count), jnp.float32)
    for p, row in enumerate(rows):
        placer = jnp.where((row_at == row) & (tok_at == p // 2), 1.0, placer)
    packed = jnp.dot(
        placer.astype(jnp.bfloat16), tok_ref[...], preferred_element_type=jnp.float32
    ).astype(jnp.bfloat16)
    for e in range(experts):
        packed_ref[e] = packed[e * CAP : (e + 1) * CAP]
    load_s.wait()
    load_c.wait()
    for m in range(moves):
        slot = slots_ref[here, m, 0]
        dest = slots_ref[here, m, 1]

        @pl.when(slot >= 0)
        def _():
            s_pay[m] = s_buf[slot]
            s_buf[slot] = jnp.zeros_like(s_pay[m])
            pltpu.make_async_copy(s_pay.at[m], send_state.at[dest], pay_sem.at[m]).start()

        for j in range(per_request):
            block = blocks_ref[here, m, 0, j]

            @pl.when(block >= 0)
            def _():
                value = c_buf[block]
                position = j * block_len + lax.broadcasted_iota(jnp.int32, value.shape, 1)
                c_pay[m, j] = jnp.where(
                    position < len_ref[here, m], value.astype(jnp.float32), 0.0
                ).astype(value.dtype)
                c_buf[block] = jnp.zeros_like(value)
                pltpu.make_async_copy(
                    c_pay.at[m, j], send_cache.at[dest, j], cpay_sem.at[m, j]
                ).start()

    store_s = pltpu.make_async_copy(s_buf, base_states, store_sem.at[0])
    store_c = pltpu.make_async_copy(c_buf, base_cache, store_sem.at[1])
    store_s.start()
    store_c.start()
    for m in range(moves):
        slot = slots_ref[here, m, 0]
        dest = slots_ref[here, m, 1]

        @pl.when(slot >= 0)
        def _():
            pltpu.make_async_copy(s_pay.at[m], send_state.at[dest], pay_sem.at[m]).wait()

        for j in range(per_request):

            @pl.when(blocks_ref[here, m, 0, j] >= 0)
            def _():
                pltpu.make_async_copy(
                    c_pay.at[m, j], send_cache.at[dest, j], cpay_sem.at[m, j]
                ).wait()

    store_s.wait()
    store_c.wait()


def land_kernel(
    slots_ref, blocks_ref, got_state, got_cache, base_states, base_cache,
    new_states, new_cache, s_buf, c_buf, in_s, in_c, out_s, out_c,
):
    here = lax.axis_index("dp")
    ranks, moves = slots_ref.shape[0], slots_ref.shape[1]
    per_request = blocks_ref.shape[3]
    plan = []
    for m in range(moves):
        anchor, arriving = jnp.int32(0), jnp.int32(0)
        for r in range(ranks):
            hit = slots_ref[r, m, 1] == here
            anchor = jnp.where(hit, r, anchor)
            arriving = jnp.where(hit, 1, arriving)
        lands = [
            (arriving > 0) & (blocks_ref[anchor, m, 1, j] >= 0) for j in range(per_request)
        ]
        plan.append((anchor, arriving > 0, lands))
    for phase in range(3):
        for m, (anchor, arriving, lands) in enumerate(plan):
            load = pltpu.make_async_copy(got_state.at[anchor], s_buf.at[m], in_s.at[m])
            place = jnp.maximum(slots_ref[anchor, m, 2], 0)
            store = pltpu.make_async_copy(s_buf.at[m], new_states.at[place], out_s.at[m])

            @pl.when(arriving)
            def _():
                if phase == 0:
                    load.start()
                elif phase == 1:
                    load.wait()
                    store.start()
                else:
                    store.wait()

            for j in range(per_request):
                cload = pltpu.make_async_copy(
                    got_cache.at[anchor, j], c_buf.at[m, j], in_c.at[m, j]
                )
                spot = jnp.maximum(blocks_ref[anchor, m, 1, j], 0)
                cstore = pltpu.make_async_copy(
                    c_buf.at[m, j], new_cache.at[spot], out_c.at[m, j]
                )

                @pl.when(lands[j])
                def _():
                    if phase == 0:
                        cload.start()
                    elif phase == 1:
                        cload.wait()
                        cstore.start()
                    else:
                        cstore.wait()


def expert_kernel(
    ranks, quads,
    ids_ref, logits_ref, packed_ref, gate_ref, up_ref, down_ref, send_state, send_cache,
    mixed_ref, got_state, got_cache,
    g_buf, u_buf, d_buf, x_in, x_all, hidden, send_buf, recv_buf,
    g_sem, u_sem, d_sem, own_sem, first_send, first_recv, second_send, second_recv,
    back_send, back_recv, mig_send, mig_recv,
):
    d = lax.axis_index("dp")
    e = lax.axis_index("ep")
    devices = ranks * quads
    me = d * quads + e
    up_tiles = gate_ref.shape[2] // UP_TILE
    down_tiles = down_ref.shape[2] // DOWN_TILE
    ring = g_buf.shape[0]
    experts = ranks

    def up_copies(j, slot):
        columns = pl.ds(pl.multiple_of(j * UP_TILE, UP_TILE), UP_TILE)
        return (
            pltpu.make_async_copy(gate_ref.at[0, :, columns], g_buf.at[slot], g_sem.at[slot]),
            pltpu.make_async_copy(up_ref.at[0, :, columns], u_buf.at[slot], u_sem.at[slot]),
        )

    def down_copy(c):
        columns = pl.ds(pl.multiple_of(c * DOWN_TILE, DOWN_TILE), DOWN_TILE)
        return pltpu.make_async_copy(down_ref.at[0, :, columns], d_buf.at[c], d_sem.at[c])

    for j in range(ring):
        for copy in up_copies(j, j):
            copy.start()

    barrier = pltpu.get_barrier_semaphore()

    @pl.loop(1, devices)
    def _(k):
        other = lax.rem(me + k, devices)
        pl.semaphore_signal(
            barrier, inc=1, device_id=(other // quads, lax.rem(other, quads)), device_id_type=MESH
        )

    pl.semaphore_wait(barrier, devices - 1)

    own = pltpu.make_async_copy(packed_ref.at[d], x_in.at[me], own_sem)
    own.start()
    for k in range(1, ranks):
        peer = lax.rem(d + k, ranks)
        pltpu.make_async_remote_copy(
            packed_ref.at[peer], x_in.at[me], first_send, first_recv.at[k],
            device_id=(peer, e), device_id_type=MESH,
        ).start()

    def forward(src, slot):
        for k in range(1, quads):
            pltpu.make_async_remote_copy(
                src, x_in.at[slot], second_send, second_recv,
                device_id=(d, lax.rem(e + k, quads)), device_id_type=MESH,
            ).start()

    forward(packed_ref.at[d], me)

    tok_count = logits_ref.shape[0]
    picks, rows = target_rows(ids_ref, tok_count)
    logits = logits_ref[...]
    lane = lax.broadcasted_iota(jnp.int32, logits.shape, 1)
    seat = lax.broadcasted_iota(jnp.int32, logits.shape, 0)
    column = lax.broadcasted_iota(jnp.int32, (tok_count, devices * CAP), 1)
    token = lax.broadcasted_iota(jnp.int32, (tok_count, devices * CAP), 0)
    row_of = (column // (quads * CAP)) * CAP + lax.rem(column, CAP)
    scores, hits = [], []
    for k in range(2):
        chosen = jnp.zeros(logits.shape, jnp.int32)
        target = jnp.zeros(column.shape, jnp.int32)
        for t in range(tok_count):
            chosen = jnp.where(seat == t, picks[2 * t + k], chosen)
            target = jnp.where(token == t, rows[2 * t + k], target)
        value = jnp.sum(jnp.where(lane == chosen, logits, 0.0), axis=1, keepdims=True)
        scores.append(jax.nn.sigmoid(value))
        hits.append(row_of == target)
    total = scores[0] + scores[1]
    comb = jnp.where(hits[0], scores[0] / total, 0.0) + jnp.where(hits[1], scores[1] / total, 0.0)
    comb_high = comb.astype(jnp.bfloat16)
    comb_low = (comb - comb_high.astype(jnp.float32)).astype(jnp.bfloat16)

    for k in range(1, ranks):
        source = lax.rem(d - k + ranks, ranks)
        slot = source * quads + e
        pltpu.make_async_remote_copy(
            x_in.at[slot], x_in.at[slot], first_send, first_recv.at[k],
            device_id=(source, e), device_id_type=MESH,
        ).wait_recv()
        forward(x_in.at[slot], slot)
    own.wait()
    arrivals = ranks * (quads - 1)
    pltpu.make_async_copy(
        x_in.at[pl.ds(0, arrivals)], x_in.at[pl.ds(0, arrivals)], second_recv
    ).wait()
    for o in range(devices):
        x_all[o * CAP : (o + 1) * CAP, :] = x_in[o]

    for k in range(1, ranks):
        peer = lax.rem(d + k, ranks)
        for i, (src, dst) in enumerate(((send_state, got_state), (send_cache, got_cache))):
            pltpu.make_async_remote_copy(
                src.at[peer], dst.at[d], mig_send.at[i], mig_recv.at[i],
                device_id=(peer, e), device_id_type=MESH,
            ).start()

    @pl.loop(0, up_tiles)
    def _(j):
        slot = lax.rem(j, ring)
        for copy in up_copies(j, slot):
            copy.wait()
        gate = jnp.dot(x_all[...], g_buf[slot], preferred_element_type=jnp.float32)
        upper = jnp.dot(x_all[...], u_buf[slot], preferred_element_type=jnp.float32)
        value = gate / (1.0 + jnp.exp(-gate)) * upper
        hidden[:, pl.ds(pl.multiple_of(j * UP_TILE, UP_TILE), UP_TILE)] = value.astype(jnp.bfloat16)

        @pl.when(j < up_tiles - ring)
        def _():
            for copy in up_copies(j + ring, slot):
                copy.start()

        @pl.when(j < down_tiles)
        def _():
            down_copy(j).start()

    @pl.loop(0, down_tiles)
    def _(c):
        down_copy(c).wait()
        part = jnp.dot(hidden[...], d_buf[c], preferred_element_type=jnp.float32)
        for o in range(devices):
            send_buf[c, o] = part[o * CAP : (o + 1) * CAP].astype(jnp.bfloat16)
        recv_buf[c, me] = send_buf[c, me]

        @pl.loop(1, devices)
        def _(k):
            other = lax.rem(me + k, devices)
            pltpu.make_async_remote_copy(
                send_buf.at[c, other], recv_buf.at[c, me], back_send.at[c], back_recv.at[c],
                device_id=(other // quads, lax.rem(other, quads)), device_id_type=MESH,
            ).start()

    @pl.loop(0, down_tiles)
    def _(c):
        most = recv_buf.at[c, pl.ds(0, devices - 1)]
        pltpu.make_async_copy(most, most, back_recv.at[c]).wait()
        rows_in = jnp.concatenate([recv_buf[c, o] for o in range(devices)], axis=0)
        high = jnp.dot(comb_high, rows_in, preferred_element_type=jnp.float32)
        low = jnp.dot(comb_low, rows_in, preferred_element_type=jnp.float32)
        mixed_ref[:, pl.ds(pl.multiple_of(c * DOWN_TILE, DOWN_TILE), DOWN_TILE)] = (
            high + low
        ).astype(jnp.bfloat16)

    for i, dst in enumerate((got_state, got_cache)):
        most = dst.at[pl.ds(0, ranks - 1)]
        pltpu.make_async_copy(most, most, mig_recv.at[i]).wait()
        pltpu.make_async_copy(most, most, mig_send.at[i]).wait()
    most = x_in.at[pl.ds(0, ranks - 1)]
    pltpu.make_async_copy(most, most, first_send).wait()
    most = x_in.at[pl.ds(0, arrivals)]
    pltpu.make_async_copy(most, most, second_send).wait()

    @pl.loop(0, down_tiles)
    def _(c):
        most = send_buf.at[c, pl.ds(0, devices - 1)]
        pltpu.make_async_copy(most, most, back_send.at[c]).wait()


def fused(
    tokens, router, expert_ids, w_gate, w_up, w_down, states, kv_blocks,
    plan_slots, plan_len, plan_blocks,
):
    ranks, quads = lax.axis_size("dp"), lax.axis_size("ep")
    devices = ranks * quads
    experts = router.shape[1]
    tok_count, width = tokens.shape
    moves = plan_slots.shape[1]
    per_request = plan_blocks.shape[3]
    bf16 = jnp.bfloat16
    dma = pltpu.SemaphoreType.DMA
    like = jax.ShapeDtypeStruct
    state_one, cache_one = states.shape[1:], kv_blocks.shape[1:]
    packed, send_state, send_cache, base_states, base_cache = pl.pallas_call(
        prepare_kernel,
        out_shape=(
            like((experts, CAP, width), bf16),
            like((ranks, *state_one), bf16),
            like((ranks, per_request, *cache_one), bf16),
            like(states.shape, bf16),
            like(kv_blocks.shape, bf16),
        ),
        in_specs=[SMEM] * 4 + [VMEM, ANY, ANY],
        out_specs=(VMEM, ANY, ANY, ANY, ANY),
        scratch_shapes=[
            pltpu.VMEM(states.shape, bf16),
            pltpu.VMEM(kv_blocks.shape, bf16),
            pltpu.VMEM((moves, *state_one), bf16),
            pltpu.VMEM((moves, per_request, *cache_one), bf16),
            dma((2,)), dma((moves,)), dma((moves, per_request)), dma((2,)),
        ],
        name="prepare",
    )(expert_ids, plan_slots, plan_len, plan_blocks, tokens, states, kv_blocks)
    logits = jnp.dot(tokens.astype(jnp.float32), router, precision=lax.Precision.HIGHEST)
    depth = w_gate.shape[2]
    ring = min(RING, depth // UP_TILE)
    down_tiles = width // DOWN_TILE
    mixed, got_state, got_cache = pl.pallas_call(
        functools.partial(expert_kernel, ranks, quads),
        out_shape=(
            like((tok_count, width), bf16),
            like((ranks, *state_one), bf16),
            like((ranks, per_request, *cache_one), bf16),
        ),
        in_specs=[SMEM, VMEM, VMEM, ANY, ANY, ANY, ANY, ANY],
        out_specs=(VMEM, ANY, ANY),
        scratch_shapes=[
            pltpu.VMEM((ring, width, UP_TILE), bf16),
            pltpu.VMEM((ring, width, UP_TILE), bf16),
            pltpu.VMEM((down_tiles, depth, DOWN_TILE), bf16),
            pltpu.VMEM((devices, CAP, width), bf16),
            pltpu.VMEM((devices * CAP, width), bf16),
            pltpu.VMEM((devices * CAP, depth), bf16),
            pltpu.VMEM((down_tiles, devices, CAP, DOWN_TILE), bf16),
            pltpu.VMEM((down_tiles, devices, CAP, DOWN_TILE), bf16),
            dma((ring,)), dma((ring,)), dma((down_tiles,)), dma,
            dma, dma((ranks,)), dma, dma,
            dma((down_tiles,)), dma((down_tiles,)), dma((2,)), dma((2,)),
        ],
        compiler_params=pltpu.CompilerParams(
            collective_id=0, has_side_effects=True, vmem_limit_bytes=VMEM_LIMIT
        ),
        name="expert",
    )(expert_ids, logits, packed, w_gate, w_up, w_down, send_state, send_cache)
    new_states, new_cache = pl.pallas_call(
        land_kernel,
        out_shape=(like(states.shape, bf16), like(kv_blocks.shape, bf16)),
        in_specs=[SMEM, SMEM, ANY, ANY, ANY, ANY],
        out_specs=(ANY, ANY),
        input_output_aliases={4: 0, 5: 1},
        scratch_shapes=[
            pltpu.VMEM((moves, *state_one), bf16),
            pltpu.VMEM((moves, per_request, *cache_one), bf16),
            dma((moves,)), dma((moves, per_request)), dma((moves,)), dma((moves, per_request)),
        ],
        name="land",
    )(plan_slots, plan_blocks, got_state, got_cache, base_states, base_cache)
    return mixed, new_states, new_cache


def local(
    tokens,
    router,
    expert_ids,
    w_gate,
    w_up,
    w_down,
    states,
    kv_blocks,
    plan_slots,
    plan_len,
    plan_blocks,
):
    ranks = lax.axis_size("dp")
    here = lax.axis_index("dp")
    moves = plan_slots.shape[1]
    slot_count = states.shape[0]
    block_count = kv_blocks.shape[0]
    per_request = plan_blocks.shape[3]
    block_len = kv_blocks.shape[2]
    mine = lax.dynamic_index_in_dim(plan_slots, here, 0, keepdims=False)
    my_blocks = lax.dynamic_index_in_dim(plan_blocks, here, 0, keepdims=False)
    my_length = lax.dynamic_index_in_dim(plan_len, here, 0, keepdims=False)
    leaving_slot = mine[:, 0]
    leaving_block = my_blocks[:, 0, :]
    state_out = states[jnp.maximum(leaving_slot, 0)]
    state_out = jnp.where((leaving_slot >= 0)[:, None, None], state_out, jnp.zeros_like(state_out))
    cache_out = kv_blocks[jnp.maximum(leaving_block, 0)]
    position = jnp.arange(per_request)[:, None] * block_len + jnp.arange(block_len)[None, :]
    written = (leaving_block >= 0)[:, :, None] & (position[None] < my_length[:, None, None])
    cache_out = jnp.where(written[:, :, None, :, None], cache_out, jnp.zeros_like(cache_out))
    arrivals = plan_slots[:, :, 1] == here
    sender = jnp.sum(jnp.where(arrivals, jnp.arange(ranks)[:, None], 0), axis=0)
    arriving = jnp.any(arrivals, axis=0)
    peers = jnp.arange(ranks)
    match = mine[:, 1][None, :] == peers[:, None]
    which = jnp.sum(jnp.where(match, jnp.arange(moves)[None, :], 0), axis=1)
    filled = jnp.any(match, axis=1)
    send_state = jnp.where(
        filled[:, None, None], state_out[which], jnp.zeros_like(state_out[which])
    )
    send_cache = jnp.where(
        filled[:, None, None, None, None], cache_out[which], jnp.zeros_like(cache_out[which])
    )
    got_state, got_cache = (
        lax.all_to_all(send_state, "dp", split_axis=0, concat_axis=0, tiled=True),
        lax.all_to_all(send_cache, "dp", split_axis=0, concat_axis=0, tiled=True),
    )
    state_in = got_state[sender]
    cache_in = got_cache[sender]
    slot_line = jnp.arange(slot_count)
    gone = jnp.any(slot_line[:, None] == leaving_slot[None, :], axis=1)
    new_states = jnp.where(gone[:, None, None], jnp.zeros_like(states), states)
    block_line = jnp.arange(block_count)
    gone_blocks = jnp.any(block_line[:, None, None] == leaving_block[None], axis=(1, 2))
    new_cache = jnp.where(gone_blocks[:, None, None, None], jnp.zeros_like(kv_blocks), kv_blocks)
    for move_index in range(moves):
        anchor = sender[move_index]
        place = plan_slots[anchor, move_index, 2]
        landing = (slot_line == place) & arriving[move_index]
        new_states = jnp.where(landing[:, None, None], state_in[move_index][None], new_states)
        for block_index in range(per_request):
            spot = plan_blocks[anchor, move_index, 1, block_index]
            block_hit = (block_line == spot) & arriving[move_index]
            new_cache = jnp.where(
                block_hit[:, None, None, None], cache_in[move_index, block_index][None], new_cache
            )
    experts = router.shape[1]
    tok_count = tokens.shape[0]
    width = tokens.shape[1]
    group = ranks // experts
    flat_ids = expert_ids.reshape(-1)
    onehot = (flat_ids[:, None] == jnp.arange(experts)[None, :]).astype(jnp.int32)
    earlier = jnp.cumsum(onehot, axis=0) - onehot
    slot_of = jnp.sum(earlier * onehot, axis=1)
    target_row = flat_ids * CAP + slot_of
    placer = (jnp.arange(experts * CAP)[:, None] == target_row[None, :]).astype(jnp.bfloat16)
    doubled = jnp.repeat(tokens, 2, axis=0)
    packed = jnp.dot(placer, doubled, preferred_element_type=jnp.float32).astype(jnp.bfloat16)
    outgoing = jnp.repeat(packed.reshape(experts, CAP, width), group, axis=0)
    incoming = lax.all_to_all(outgoing, "dp", split_axis=0, concat_axis=0, tiled=True)
    rows_in = incoming.reshape(ranks * CAP, width)
    piece = lax.all_gather(rows_in, "ep", axis=0, tiled=True)
    gate = jnp.dot(piece, w_gate[0], preferred_element_type=jnp.float32)
    upper = jnp.dot(piece, w_up[0], preferred_element_type=jnp.float32)
    hidden = (jax.nn.silu(gate) * upper).astype(jnp.bfloat16)
    summed = lax.psum_scatter(
        jnp.dot(hidden, w_down[0], preferred_element_type=jnp.float32),
        "ep",
        scatter_dimension=0,
        tiled=True,
    )
    returned = lax.all_to_all(
        summed.reshape(ranks, CAP, width), "dp", split_axis=0, concat_axis=0, tiled=True
    )
    expert_out = jnp.sum(returned.reshape(experts, group, CAP, width), axis=1).reshape(
        experts * CAP, width
    )
    chosen = expert_out[target_row].reshape(tok_count, 2, width)
    logits = jnp.dot(tokens.astype(jnp.float32), router, precision=lax.Precision.HIGHEST)
    scores = jax.nn.sigmoid(jnp.take_along_axis(logits, expert_ids, axis=1))
    weights = scores / jnp.sum(scores, axis=1, keepdims=True)
    mixed = jnp.sum(weights[:, :, None] * chosen, axis=1).astype(jnp.bfloat16)
    return (mixed, new_states, new_cache)


def solution(mesh):
    placed = (
        P(("dp", "ep"), None),
        P(),
        P(("dp", "ep"), None),
        P("dp", None, "ep"),
        P("dp", None, "ep"),
        P("dp", "ep", None),
        P("dp", None, "ep"),
        P("dp", None, None, "ep"),
        P(),
        P(),
        P(),
    )
    def step(*args):
        one_slab = args[1].shape[1] == lax.axis_size("dp")
        return (fused if one_slab else local)(*args)

    return jax.shard_map(
        step,
        mesh=mesh,
        in_specs=placed,
        out_specs=(P(("dp", "ep"), None), P("dp", None, "ep"), P("dp", None, None, "ep")),
        check_vma=False,
    )
```

```python
import functools

import jax
import jax.numpy as jnp
from jax import lax
from jax.experimental import pallas as pl
from jax.experimental.pallas import tpu as pltpu
from jax.sharding import PartitionSpec as P

CAP = 2
MESH = pl.DeviceIdType.MESH
ANY = pl.BlockSpec(memory_space=pl.ANY)
VMEM = pl.BlockSpec(memory_space=pltpu.VMEM)
SMEM = pl.BlockSpec(memory_space=pltpu.SMEM)
VMEM_LIMIT = 67_000_000
UP_TILE = 256
DOWN_TILE = 512
RING = 8


def target_rows(ids_ref, tok_count):
    picks = [ids_ref[k, t] for t in range(tok_count) for k in range(2)]
    rows = []
    for p, expert in enumerate(picks):
        slot = jnp.int32(0)
        for q in range(p):
            slot = slot + jnp.where(picks[q] == expert, 1, 0)
        rows.append(expert * CAP + slot)
    return picks, rows


def land_kernel(
    slots_ref, blocks_ref, got_state, got_cache, states_ref, kv_ref, part_ref,
    new_states, new_cache, mixed_ref, s_all, c_all, m_all, s_buf, c_buf,
    in_sem, in_s, in_c, out_sem,
):
    here = lax.axis_index("dp")
    moves, ranks = slots_ref.shape[1:]
    per_request = blocks_ref.shape[2]
    whole = ((states_ref, s_all, new_states), (kv_ref, c_all, new_cache), (part_ref, m_all, mixed_ref))
    loads = [pltpu.make_async_copy(a, b, in_sem.at[i]) for i, (a, b, _) in enumerate(whole)]
    stores = [pltpu.make_async_copy(b, c, out_sem.at[i]) for i, (_, b, c) in enumerate(whole)]
    for copy in loads:
        copy.start()
    plan = []
    for m in range(moves):
        anchor, arriving = jnp.int32(0), jnp.int32(0)
        for r in range(ranks):
            hit = slots_ref[1, m, r] == here
            anchor = jnp.where(hit, r, anchor)
            arriving = jnp.where(hit, 1, arriving)
        plan.append((anchor, arriving > 0))

    def state_load(m, anchor):
        return pltpu.make_async_copy(got_state.at[anchor], s_buf.at[m], in_s.at[m])

    def cache_load(m, j, anchor):
        return pltpu.make_async_copy(got_cache.at[anchor, j], c_buf.at[m, j], in_c.at[m, j])

    for m, (anchor, arriving) in enumerate(plan):

        @pl.when(arriving)
        def _():
            state_load(m, anchor).start()
            for j in range(per_request):
                cache_load(m, j, anchor).start()

    for copy in loads:
        copy.wait()
    stores[2].start()
    for m, (anchor, arriving) in enumerate(plan):
        slot = slots_ref[0, m, here]

        @pl.when(slot >= 0)
        def _():
            s_all[slot] = jnp.zeros_like(s_buf[m])

        for j in range(per_request):
            block = blocks_ref[m, 0, j, here]

            @pl.when(block >= 0)
            def _():
                c_all[block] = jnp.zeros_like(c_buf[m, j])

        @pl.when(arriving)
        def _():
            state_load(m, anchor).wait()
            s_all[slots_ref[2, m, anchor]] = s_buf[m]
            for j in range(per_request):
                cache_load(m, j, anchor).wait()
                spot = blocks_ref[m, 1, j, anchor]

                @pl.when(spot >= 0)
                def _():
                    c_all[spot] = c_buf[m, j]

    stores[0].start()
    stores[1].start()
    for copy in stores:
        copy.wait()


def expert_kernel(
    ranks, quads,
    ids_ref, slots_ref, len_ref, blocks_ref, tok_ref, router_ref, gate_ref, up_ref, down_ref,
    states_ref, kv_ref,
    mixed_ref, got_state, got_cache,
    packed_ref, s_all, c_all, s_pay, c_pay, send_state, send_cache, mig_load,
    g_buf, u_buf, d_buf, x_in, x_all, hidden, send_buf, recv_buf,
    g_sem, u_sem, d_sem, own_sem, first_send, first_recv, second_send, second_recv,
    back_send, back_recv, mig_send, mig_recv,
):
    d = lax.axis_index("dp")
    e = lax.axis_index("ep")
    devices = ranks * quads
    me = d * quads + e
    up_tiles = gate_ref.shape[2] // UP_TILE
    down_tiles = down_ref.shape[2] // DOWN_TILE
    ring = g_buf.shape[0]
    experts = ranks

    def up_copies(j, slot):
        columns = pl.ds(pl.multiple_of(j * UP_TILE, UP_TILE), UP_TILE)
        return (
            pltpu.make_async_copy(gate_ref.at[0, :, columns], g_buf.at[slot], g_sem.at[slot]),
            pltpu.make_async_copy(up_ref.at[0, :, columns], u_buf.at[slot], u_sem.at[slot]),
        )

    def down_copy(c):
        columns = pl.ds(pl.multiple_of(c * DOWN_TILE, DOWN_TILE), DOWN_TILE)
        return pltpu.make_async_copy(down_ref.at[0, :, columns], d_buf.at[c], d_sem.at[c])

    for j in range(ring):
        for copy in up_copies(j, j):
            copy.start()

    load_states = pltpu.make_async_copy(states_ref, s_all, mig_load.at[0])
    load_cache = pltpu.make_async_copy(kv_ref, c_all, mig_load.at[1])
    load_states.start()
    load_cache.start()
    for c in range(down_tiles):
        down_copy(c).start()

    barrier = pltpu.get_barrier_semaphore()

    @pl.loop(1, devices)
    def _(k):
        other = lax.rem(me + k, devices)
        pl.semaphore_signal(
            barrier, inc=1, device_id=(other // quads, lax.rem(other, quads)), device_id_type=MESH
        )

    tok_count = tok_ref.shape[0]
    picks, rows = target_rows(ids_ref, tok_count)
    row_at = lax.broadcasted_iota(jnp.int32, (experts * CAP, tok_count), 0)
    tok_at = lax.broadcasted_iota(jnp.int32, (experts * CAP, tok_count), 1)
    placer = jnp.zeros((experts * CAP, tok_count), jnp.float32)
    for p, row in enumerate(rows):
        placer = jnp.where((row_at == row) & (tok_at == p // 2), 1.0, placer)
    packed = jnp.dot(
        placer.astype(jnp.bfloat16), tok_ref[...], preferred_element_type=jnp.float32
    ).astype(jnp.bfloat16)
    for r in range(experts):
        packed_ref[r] = packed[r * CAP : (r + 1) * CAP]

    pl.semaphore_wait(barrier, devices - 1)

    own = pltpu.make_async_copy(packed_ref.at[d], x_in.at[me], own_sem)
    own.start()
    for k in range(1, ranks):
        peer = lax.rem(d + k, ranks)
        pltpu.make_async_remote_copy(
            packed_ref.at[peer], x_in.at[me], first_send, first_recv.at[k],
            device_id=(peer, e), device_id_type=MESH,
        ).start()

    def forward(src, slot):
        for k in range(1, quads):
            pltpu.make_async_remote_copy(
                src, x_in.at[slot], second_send, second_recv,
                device_id=(d, lax.rem(e + k, quads)), device_id_type=MESH,
            ).start()

    forward(packed_ref.at[d], me)

    wide = tok_ref[...].astype(jnp.float32)
    lane = lax.broadcasted_iota(jnp.int32, (tok_count, experts), 1)
    seat = lax.broadcasted_iota(jnp.int32, (tok_count, experts), 0)
    logits = jnp.zeros((tok_count, experts), jnp.float32)
    for r in range(experts):
        product = jnp.sum(wide * router_ref[r : r + 1, :], axis=1, keepdims=True)
        logits = jnp.where(lane == r, product, logits)
    column = lax.broadcasted_iota(jnp.int32, (tok_count, devices * CAP), 1)
    token = lax.broadcasted_iota(jnp.int32, (tok_count, devices * CAP), 0)
    row_of = (column // (quads * CAP)) * CAP + lax.rem(column, CAP)
    scores, hits = [], []
    for k in range(2):
        chosen = jnp.zeros(logits.shape, jnp.int32)
        target = jnp.zeros(column.shape, jnp.int32)
        for t in range(tok_count):
            chosen = jnp.where(seat == t, picks[2 * t + k], chosen)
            target = jnp.where(token == t, rows[2 * t + k], target)
        value = jnp.sum(jnp.where(lane == chosen, logits, 0.0), axis=1, keepdims=True)
        scores.append(jax.nn.sigmoid(value))
        hits.append(row_of == target)
    total = scores[0] + scores[1]
    comb = jnp.where(hits[0], scores[0] / total, 0.0) + jnp.where(hits[1], scores[1] / total, 0.0)
    comb_high = comb.astype(jnp.bfloat16)
    comb_low = (comb - comb_high.astype(jnp.float32)).astype(jnp.bfloat16)

    for k in range(1, ranks):
        source = lax.rem(d - k + ranks, ranks)
        slot = source * quads + e
        pltpu.make_async_remote_copy(
            x_in.at[slot], x_in.at[slot], first_send, first_recv.at[k],
            device_id=(source, e), device_id_type=MESH,
        ).wait_recv()
        forward(x_in.at[slot], slot)

    load_states.wait()
    load_cache.wait()
    moves = slots_ref.shape[1]
    per_request = blocks_ref.shape[2]
    block_len = kv_ref.shape[2]
    position = lax.broadcasted_iota(jnp.int32, kv_ref.shape[1:], 1)
    for m in range(moves):
        slot = slots_ref[0, m, d]
        s_pay[m] = jnp.zeros_like(s_pay[m])

        @pl.loop(0, s_all.shape[0])
        def _(s):
            s_pay[m] = lax.select(slot == s, s_all[s], s_pay[m])

        for j in range(per_request):
            block = blocks_ref[m, 0, j, d]
            c_pay[m, j] = jnp.zeros_like(c_pay[m, j])

            @pl.loop(0, c_all.shape[0])
            def _(s):
                c_pay[m, j] = lax.select(block == s, c_all[s], c_pay[m, j])

            kept = c_pay[m, j].astype(jnp.float32)
            kept = jnp.where(j * block_len + position < len_ref[m, d], kept, 0.0)
            c_pay[m, j] = kept.astype(jnp.bfloat16)
    for r in range(ranks):
        s_value, c_value = s_pay[0], c_pay[0]
        for m in range(1, moves):
            hit = slots_ref[1, m, d] == r
            s_value = lax.select(hit, s_pay[m], s_value)
            c_value = lax.select(hit, c_pay[m], c_value)
        send_state[r] = s_value
        send_cache[r] = c_value

    own.wait()
    arrivals = ranks * (quads - 1)
    pltpu.make_async_copy(
        x_in.at[pl.ds(0, arrivals)], x_in.at[pl.ds(0, arrivals)], second_recv
    ).wait()
    for o in range(devices):
        x_all[o * CAP : (o + 1) * CAP, :] = x_in[o]

    for k in range(1, ranks):
        peer = lax.rem(d + k, ranks)
        for i, (src, dst) in enumerate(((send_state, got_state), (send_cache, got_cache))):
            pltpu.make_async_remote_copy(
                src.at[peer], dst.at[d], mig_send.at[i], mig_recv.at[i],
                device_id=(peer, e), device_id_type=MESH,
            ).start()

    @pl.loop(0, up_tiles)
    def _(j):
        slot = lax.rem(j, ring)
        for copy in up_copies(j, slot):
            copy.wait()
        gate = jnp.dot(x_all[...], g_buf[slot], preferred_element_type=jnp.float32)
        upper = jnp.dot(x_all[...], u_buf[slot], preferred_element_type=jnp.float32)
        value = gate / (1.0 + jnp.exp(-gate)) * upper
        hidden[:, pl.ds(pl.multiple_of(j * UP_TILE, UP_TILE), UP_TILE)] = value.astype(jnp.bfloat16)

        @pl.when(j < up_tiles - ring)
        def _():
            for copy in up_copies(j + ring, slot):
                copy.start()

    @pl.loop(0, down_tiles)
    def _(c):
        down_copy(c).wait()
        part = jnp.dot(hidden[...], d_buf[c], preferred_element_type=jnp.float32)
        for o in range(devices):
            send_buf[c, o] = part[o * CAP : (o + 1) * CAP].astype(jnp.bfloat16)
        recv_buf[c, me] = send_buf[c, me]

        @pl.loop(1, devices)
        def _(k):
            other = lax.rem(me + k, devices)
            pltpu.make_async_remote_copy(
                send_buf.at[c, other], recv_buf.at[c, me], back_send.at[c], back_recv.at[c],
                device_id=(other // quads, lax.rem(other, quads)), device_id_type=MESH,
            ).start()

    @pl.loop(0, down_tiles)
    def _(c):
        most = recv_buf.at[c, pl.ds(0, devices - 1)]
        pltpu.make_async_copy(most, most, back_recv.at[c]).wait()
        rows_in = jnp.concatenate([recv_buf[c, o] for o in range(devices)], axis=0)
        high = jnp.dot(comb_high, rows_in, preferred_element_type=jnp.float32)
        low = jnp.dot(comb_low, rows_in, preferred_element_type=jnp.float32)
        mixed_ref[:, pl.ds(pl.multiple_of(c * DOWN_TILE, DOWN_TILE), DOWN_TILE)] = (
            high + low
        ).astype(jnp.bfloat16)

    for i, dst in enumerate((got_state, got_cache)):
        most = dst.at[pl.ds(0, ranks - 1)]
        pltpu.make_async_copy(most, most, mig_recv.at[i]).wait()
        pltpu.make_async_copy(most, most, mig_send.at[i]).wait()
    most = x_in.at[pl.ds(0, ranks - 1)]
    pltpu.make_async_copy(most, most, first_send).wait()
    most = x_in.at[pl.ds(0, arrivals)]
    pltpu.make_async_copy(most, most, second_send).wait()

    @pl.loop(0, down_tiles)
    def _(c):
        most = send_buf.at[c, pl.ds(0, devices - 1)]
        pltpu.make_async_copy(most, most, back_send.at[c]).wait()


def fused(
    tokens, router, expert_ids, w_gate, w_up, w_down, states, kv_blocks,
    plan_slots, plan_len, plan_blocks,
):
    ranks, quads = lax.axis_size("dp"), lax.axis_size("ep")
    devices = ranks * quads
    experts = router.shape[1]
    tok_count, width = tokens.shape
    moves = plan_slots.shape[1]
    per_request = plan_blocks.shape[3]
    bf16 = jnp.bfloat16
    dma = pltpu.SemaphoreType.DMA
    like = jax.ShapeDtypeStruct
    state_one, cache_one = states.shape[1:], kv_blocks.shape[1:]
    ids = expert_ids.T
    slots = jnp.transpose(plan_slots, (2, 1, 0))
    lengths = plan_len.T
    blocks = jnp.transpose(plan_blocks, (1, 2, 3, 0))
    depth = w_gate.shape[2]
    ring = min(RING, depth // UP_TILE)
    down_tiles = width // DOWN_TILE
    mixed, got_state, got_cache = pl.pallas_call(
        functools.partial(expert_kernel, ranks, quads),
        out_shape=(
            like((tok_count, width), bf16),
            like((ranks, *state_one), bf16),
            like((ranks, per_request, *cache_one), bf16),
        ),
        in_specs=[SMEM] * 4 + [VMEM] * 2 + [ANY] * 5,
        out_specs=(VMEM, ANY, ANY),
        scratch_shapes=[
            pltpu.VMEM((experts, CAP, width), bf16),
            pltpu.VMEM(states.shape, bf16),
            pltpu.VMEM(kv_blocks.shape, bf16),
            pltpu.VMEM((moves, *state_one), bf16),
            pltpu.VMEM((moves, per_request, *cache_one), bf16),
            pltpu.VMEM((ranks, *state_one), bf16),
            pltpu.VMEM((ranks, per_request, *cache_one), bf16),
            dma((2,)),
            pltpu.VMEM((ring, width, UP_TILE), bf16),
            pltpu.VMEM((ring, width, UP_TILE), bf16),
            pltpu.VMEM((down_tiles, depth, DOWN_TILE), bf16),
            pltpu.VMEM((devices, CAP, width), bf16),
            pltpu.VMEM((devices * CAP, width), bf16),
            pltpu.VMEM((devices * CAP, depth), bf16),
            pltpu.VMEM((down_tiles, devices, CAP, DOWN_TILE), bf16),
            pltpu.VMEM((down_tiles, devices, CAP, DOWN_TILE), bf16),
            dma((ring,)), dma((ring,)), dma((down_tiles,)), dma,
            dma, dma((ranks,)), dma, dma,
            dma((down_tiles,)), dma((down_tiles,)), dma((2,)), dma((2,)),
        ],
        compiler_params=pltpu.CompilerParams(
            collective_id=0, has_side_effects=True, vmem_limit_bytes=VMEM_LIMIT
        ),
        name="expert",
    )(
        ids, slots, lengths, blocks, tokens, router.T, w_gate, w_up, w_down, states, kv_blocks
    )
    new_states, new_cache, mixed = pl.pallas_call(
        land_kernel,
        out_shape=(like(states.shape, bf16), like(kv_blocks.shape, bf16), like(mixed.shape, bf16)),
        in_specs=[SMEM, SMEM] + [ANY] * 5,
        out_specs=(ANY, ANY, ANY),
        scratch_shapes=[
            pltpu.VMEM(states.shape, bf16),
            pltpu.VMEM(kv_blocks.shape, bf16),
            pltpu.VMEM(mixed.shape, bf16),
            pltpu.VMEM((moves, *state_one), bf16),
            pltpu.VMEM((moves, per_request, *cache_one), bf16),
            dma((3,)), dma((moves,)), dma((moves, per_request)), dma((3,)),
        ],
        name="land",
    )(slots, blocks, got_state, got_cache, states, kv_blocks, mixed)
    return mixed, new_states, new_cache


def local(
    tokens,
    router,
    expert_ids,
    w_gate,
    w_up,
    w_down,
    states,
    kv_blocks,
    plan_slots,
    plan_len,
    plan_blocks,
):
    ranks = lax.axis_size("dp")
    here = lax.axis_index("dp")
    moves = plan_slots.shape[1]
    slot_count = states.shape[0]
    block_count = kv_blocks.shape[0]
    per_request = plan_blocks.shape[3]
    block_len = kv_blocks.shape[2]
    mine = lax.dynamic_index_in_dim(plan_slots, here, 0, keepdims=False)
    my_blocks = lax.dynamic_index_in_dim(plan_blocks, here, 0, keepdims=False)
    my_length = lax.dynamic_index_in_dim(plan_len, here, 0, keepdims=False)
    leaving_slot = mine[:, 0]
    leaving_block = my_blocks[:, 0, :]
    state_out = states[jnp.maximum(leaving_slot, 0)]
    state_out = jnp.where((leaving_slot >= 0)[:, None, None], state_out, jnp.zeros_like(state_out))
    cache_out = kv_blocks[jnp.maximum(leaving_block, 0)]
    position = jnp.arange(per_request)[:, None] * block_len + jnp.arange(block_len)[None, :]
    written = (leaving_block >= 0)[:, :, None] & (position[None] < my_length[:, None, None])
    cache_out = jnp.where(written[:, :, None, :, None], cache_out, jnp.zeros_like(cache_out))
    arrivals = plan_slots[:, :, 1] == here
    sender = jnp.sum(jnp.where(arrivals, jnp.arange(ranks)[:, None], 0), axis=0)
    arriving = jnp.any(arrivals, axis=0)
    peers = jnp.arange(ranks)
    match = mine[:, 1][None, :] == peers[:, None]
    which = jnp.sum(jnp.where(match, jnp.arange(moves)[None, :], 0), axis=1)
    filled = jnp.any(match, axis=1)
    send_state = jnp.where(
        filled[:, None, None], state_out[which], jnp.zeros_like(state_out[which])
    )
    send_cache = jnp.where(
        filled[:, None, None, None, None], cache_out[which], jnp.zeros_like(cache_out[which])
    )
    got_state, got_cache = (
        lax.all_to_all(send_state, "dp", split_axis=0, concat_axis=0, tiled=True),
        lax.all_to_all(send_cache, "dp", split_axis=0, concat_axis=0, tiled=True),
    )
    state_in = got_state[sender]
    cache_in = got_cache[sender]
    slot_line = jnp.arange(slot_count)
    gone = jnp.any(slot_line[:, None] == leaving_slot[None, :], axis=1)
    new_states = jnp.where(gone[:, None, None], jnp.zeros_like(states), states)
    block_line = jnp.arange(block_count)
    gone_blocks = jnp.any(block_line[:, None, None] == leaving_block[None], axis=(1, 2))
    new_cache = jnp.where(gone_blocks[:, None, None, None], jnp.zeros_like(kv_blocks), kv_blocks)
    for move_index in range(moves):
        anchor = sender[move_index]
        place = plan_slots[anchor, move_index, 2]
        landing = (slot_line == place) & arriving[move_index]
        new_states = jnp.where(landing[:, None, None], state_in[move_index][None], new_states)
        for block_index in range(per_request):
            spot = plan_blocks[anchor, move_index, 1, block_index]
            block_hit = (block_line == spot) & arriving[move_index]
            new_cache = jnp.where(
                block_hit[:, None, None, None], cache_in[move_index, block_index][None], new_cache
            )
    experts = router.shape[1]
    tok_count = tokens.shape[0]
    width = tokens.shape[1]
    group = ranks // experts
    flat_ids = expert_ids.reshape(-1)
    onehot = (flat_ids[:, None] == jnp.arange(experts)[None, :]).astype(jnp.int32)
    earlier = jnp.cumsum(onehot, axis=0) - onehot
    slot_of = jnp.sum(earlier * onehot, axis=1)
    target_row = flat_ids * CAP + slot_of
    placer = (jnp.arange(experts * CAP)[:, None] == target_row[None, :]).astype(jnp.bfloat16)
    doubled = jnp.repeat(tokens, 2, axis=0)
    packed = jnp.dot(placer, doubled, preferred_element_type=jnp.float32).astype(jnp.bfloat16)
    outgoing = jnp.repeat(packed.reshape(experts, CAP, width), group, axis=0)
    incoming = lax.all_to_all(outgoing, "dp", split_axis=0, concat_axis=0, tiled=True)
    rows_in = incoming.reshape(ranks * CAP, width)
    piece = lax.all_gather(rows_in, "ep", axis=0, tiled=True)
    gate = jnp.dot(piece, w_gate[0], preferred_element_type=jnp.float32)
    upper = jnp.dot(piece, w_up[0], preferred_element_type=jnp.float32)
    hidden = (jax.nn.silu(gate) * upper).astype(jnp.bfloat16)
    summed = lax.psum_scatter(
        jnp.dot(hidden, w_down[0], preferred_element_type=jnp.float32),
        "ep",
        scatter_dimension=0,
        tiled=True,
    )
    returned = lax.all_to_all(
        summed.reshape(ranks, CAP, width), "dp", split_axis=0, concat_axis=0, tiled=True
    )
    expert_out = jnp.sum(returned.reshape(experts, group, CAP, width), axis=1).reshape(
        experts * CAP, width
    )
    chosen = expert_out[target_row].reshape(tok_count, 2, width)
    logits = jnp.dot(tokens.astype(jnp.float32), router, precision=lax.Precision.HIGHEST)
    scores = jax.nn.sigmoid(jnp.take_along_axis(logits, expert_ids, axis=1))
    weights = scores / jnp.sum(scores, axis=1, keepdims=True)
    mixed = jnp.sum(weights[:, :, None] * chosen, axis=1).astype(jnp.bfloat16)
    return (mixed, new_states, new_cache)


def solution(mesh):
    placed = (
        P(("dp", "ep"), None),
        P(),
        P(("dp", "ep"), None),
        P("dp", None, "ep"),
        P("dp", None, "ep"),
        P("dp", "ep", None),
        P("dp", None, "ep"),
        P("dp", None, None, "ep"),
        P(),
        P(),
        P(),
    )
    def step(*args):
        one_slab = args[1].shape[1] == lax.axis_size("dp")
        return (fused if one_slab else local)(*args)

    return jax.shard_map(
        step,
        mesh=mesh,
        in_specs=placed,
        out_specs=(P(("dp", "ep"), None), P("dp", None, "ep"), P("dp", None, None, "ep")),
        check_vma=False,
    )
```

```python
import functools

import jax
import jax.numpy as jnp
from jax import lax
from jax.experimental import pallas as pl
from jax.experimental.pallas import tpu as pltpu
from jax.sharding import PartitionSpec as P

CAP = 2
MESH = pl.DeviceIdType.MESH
ANY = pl.BlockSpec(memory_space=pl.ANY)
VMEM = pl.BlockSpec(memory_space=pltpu.VMEM)
SMEM = pl.BlockSpec(memory_space=pltpu.SMEM)
VMEM_LIMIT = 67_000_000
UP_TILE = 256
DOWN_TILE = 512
RING = 8


def target_rows(ids_ref, tok_count):
    picks = [ids_ref[k, t] for t in range(tok_count) for k in range(2)]
    rows = []
    for p, expert in enumerate(picks):
        slot = jnp.int32(0)
        for q in range(p):
            slot = slot + jnp.where(picks[q] == expert, 1, 0)
        rows.append(expert * CAP + slot)
    return picks, rows


def land_kernel(
    slots_ref, blocks_ref, got_state, got_cache, states_ref, kv_ref, part_ref,
    new_states, new_cache, mixed_ref, s_all, c_all, m_all, s_buf, c_buf,
    in_sem, in_s, in_c, out_sem,
):
    here = lax.axis_index("dp")
    moves, ranks = slots_ref.shape[1:]
    per_request = blocks_ref.shape[2]
    whole = ((states_ref, s_all, new_states), (kv_ref, c_all, new_cache), (part_ref, m_all, mixed_ref))
    loads = [pltpu.make_async_copy(a, b, in_sem.at[i]) for i, (a, b, _) in enumerate(whole)]
    stores = [pltpu.make_async_copy(b, c, out_sem.at[i]) for i, (_, b, c) in enumerate(whole)]
    for copy in loads:
        copy.start()
    plan = []
    for m in range(moves):
        anchor, arriving = jnp.int32(0), jnp.int32(0)
        for r in range(ranks):
            hit = slots_ref[1, m, r] == here
            anchor = jnp.where(hit, r, anchor)
            arriving = jnp.where(hit, 1, arriving)
        plan.append((anchor, arriving > 0))

    def state_load(m, anchor):
        return pltpu.make_async_copy(got_state.at[anchor], s_buf.at[m], in_s.at[m])

    def cache_load(m, j, anchor):
        return pltpu.make_async_copy(got_cache.at[anchor, j], c_buf.at[m, j], in_c.at[m, j])

    for m, (anchor, arriving) in enumerate(plan):

        @pl.when(arriving)
        def _():
            state_load(m, anchor).start()
            for j in range(per_request):
                cache_load(m, j, anchor).start()

    for copy in loads:
        copy.wait()
    stores[2].start()
    for m, (anchor, arriving) in enumerate(plan):
        slot = slots_ref[0, m, here]

        @pl.when(slot >= 0)
        def _():
            s_all[slot] = jnp.zeros_like(s_buf[m])

        for j in range(per_request):
            block = blocks_ref[m, 0, j, here]

            @pl.when(block >= 0)
            def _():
                c_all[block] = jnp.zeros_like(c_buf[m, j])

        @pl.when(arriving)
        def _():
            state_load(m, anchor).wait()
            s_all[slots_ref[2, m, anchor]] = s_buf[m]
            for j in range(per_request):
                cache_load(m, j, anchor).wait()
                spot = blocks_ref[m, 1, j, anchor]

                @pl.when(spot >= 0)
                def _():
                    c_all[spot] = c_buf[m, j]

    stores[0].start()
    stores[1].start()
    for copy in stores:
        copy.wait()


def expert_kernel(
    ranks, quads,
    ids_ref, slots_ref, len_ref, blocks_ref, tok_ref, router_ref, gate_ref, up_ref, down_ref,
    states_ref, kv_ref,
    mixed_ref, got_state, got_cache,
    packed_ref, s_all, c_all, s_pay, c_pay, send_state, send_cache, mig_load,
    g_buf, u_buf, d_buf, x_in, x_all, hidden, send_buf, recv_buf,
    g_sem, u_sem, d_sem, own_sem, first_send, first_recv, second_send, second_recv,
    back_send, back_recv, mig_send, mig_recv,
):
    d = lax.axis_index("dp")
    e = lax.axis_index("ep")
    devices = ranks * quads
    me = d * quads + e
    up_tiles = gate_ref.shape[2] // UP_TILE
    down_tiles = down_ref.shape[2] // DOWN_TILE
    ring = g_buf.shape[0]
    experts = ranks

    def up_copies(j, slot):
        columns = pl.ds(pl.multiple_of(j * UP_TILE, UP_TILE), UP_TILE)
        return (
            pltpu.make_async_copy(gate_ref.at[0, :, columns], g_buf.at[slot], g_sem.at[slot]),
            pltpu.make_async_copy(up_ref.at[0, :, columns], u_buf.at[slot], u_sem.at[slot]),
        )

    def down_copy(c):
        columns = pl.ds(pl.multiple_of(c * DOWN_TILE, DOWN_TILE), DOWN_TILE)
        return pltpu.make_async_copy(down_ref.at[0, :, columns], d_buf.at[c], d_sem.at[c])

    load_states = pltpu.make_async_copy(states_ref, s_all, mig_load.at[0])
    load_cache = pltpu.make_async_copy(kv_ref, c_all, mig_load.at[1])
    load_states.start()
    load_cache.start()
    for j in range(ring):
        for copy in up_copies(j, j):
            copy.start()

    for c in range(down_tiles):
        down_copy(c).start()

    barrier = pltpu.get_barrier_semaphore()

    @pl.loop(1, devices)
    def _(k):
        other = lax.rem(me + k, devices)
        pl.semaphore_signal(
            barrier, inc=1, device_id=(other // quads, lax.rem(other, quads)), device_id_type=MESH
        )

    tok_count = tok_ref.shape[0]
    picks, rows = target_rows(ids_ref, tok_count)
    row_at = lax.broadcasted_iota(jnp.int32, (experts * CAP, tok_count), 0)
    tok_at = lax.broadcasted_iota(jnp.int32, (experts * CAP, tok_count), 1)
    placer = jnp.zeros((experts * CAP, tok_count), jnp.float32)
    for p, row in enumerate(rows):
        placer = jnp.where((row_at == row) & (tok_at == p // 2), 1.0, placer)
    packed = jnp.dot(
        placer.astype(jnp.bfloat16), tok_ref[...], preferred_element_type=jnp.float32
    ).astype(jnp.bfloat16)
    for r in range(experts):
        packed_ref[r] = packed[r * CAP : (r + 1) * CAP]

    pl.semaphore_wait(barrier, devices - 1)

    own = pltpu.make_async_copy(packed_ref.at[d], x_in.at[me], own_sem)
    own.start()
    for k in range(1, ranks):
        peer = lax.rem(d + k, ranks)
        pltpu.make_async_remote_copy(
            packed_ref.at[peer], x_in.at[me], first_send, first_recv.at[k],
            device_id=(peer, e), device_id_type=MESH,
        ).start()

    def forward(src, slot):
        for k in range(1, quads):
            pltpu.make_async_remote_copy(
                src, x_in.at[slot], second_send, second_recv,
                device_id=(d, lax.rem(e + k, quads)), device_id_type=MESH,
            ).start()

    forward(packed_ref.at[d], me)

    wide = tok_ref[...].astype(jnp.float32)
    lane = lax.broadcasted_iota(jnp.int32, (tok_count, experts), 1)
    seat = lax.broadcasted_iota(jnp.int32, (tok_count, experts), 0)
    logits = jnp.zeros((tok_count, experts), jnp.float32)
    for r in range(experts):
        product = jnp.sum(wide * router_ref[r : r + 1, :], axis=1, keepdims=True)
        logits = jnp.where(lane == r, product, logits)
    column = lax.broadcasted_iota(jnp.int32, (tok_count, devices * CAP), 1)
    token = lax.broadcasted_iota(jnp.int32, (tok_count, devices * CAP), 0)
    row_of = (column // (quads * CAP)) * CAP + lax.rem(column, CAP)
    scores, hits = [], []
    for k in range(2):
        chosen = jnp.zeros(logits.shape, jnp.int32)
        target = jnp.zeros(column.shape, jnp.int32)
        for t in range(tok_count):
            chosen = jnp.where(seat == t, picks[2 * t + k], chosen)
            target = jnp.where(token == t, rows[2 * t + k], target)
        value = jnp.sum(jnp.where(lane == chosen, logits, 0.0), axis=1, keepdims=True)
        scores.append(jax.nn.sigmoid(value))
        hits.append(row_of == target)
    total = scores[0] + scores[1]
    comb = jnp.where(hits[0], scores[0] / total, 0.0) + jnp.where(hits[1], scores[1] / total, 0.0)
    comb_high = comb.astype(jnp.bfloat16)
    comb_low = (comb - comb_high.astype(jnp.float32)).astype(jnp.bfloat16)

    for k in range(1, ranks):
        source = lax.rem(d - k + ranks, ranks)
        slot = source * quads + e
        pltpu.make_async_remote_copy(
            x_in.at[slot], x_in.at[slot], first_send, first_recv.at[k],
            device_id=(source, e), device_id_type=MESH,
        ).wait_recv()
        forward(x_in.at[slot], slot)

    load_states.wait()
    load_cache.wait()
    moves = slots_ref.shape[1]
    per_request = blocks_ref.shape[2]
    block_len = kv_ref.shape[2]
    position = lax.broadcasted_iota(jnp.int32, kv_ref.shape[1:], 1)
    for m in range(moves):
        slot = slots_ref[0, m, d]
        s_pay[m] = jnp.zeros_like(s_pay[m])

        @pl.loop(0, s_all.shape[0])
        def _(s):
            s_pay[m] = lax.select(slot == s, s_all[s], s_pay[m])

        for j in range(per_request):
            block = blocks_ref[m, 0, j, d]
            c_pay[m, j] = jnp.zeros_like(c_pay[m, j])

            @pl.loop(0, c_all.shape[0])
            def _(s):
                c_pay[m, j] = lax.select(block == s, c_all[s], c_pay[m, j])

            kept = c_pay[m, j].astype(jnp.float32)
            kept = jnp.where(j * block_len + position < len_ref[m, d], kept, 0.0)
            c_pay[m, j] = kept.astype(jnp.bfloat16)
    for r in range(ranks):
        s_value, c_value = s_pay[0], c_pay[0]
        for m in range(1, moves):
            hit = slots_ref[1, m, d] == r
            s_value = lax.select(hit, s_pay[m], s_value)
            c_value = lax.select(hit, c_pay[m], c_value)
        send_state[r] = s_value
        send_cache[r] = c_value

    own.wait()
    arrivals = ranks * (quads - 1)
    pltpu.make_async_copy(
        x_in.at[pl.ds(0, arrivals)], x_in.at[pl.ds(0, arrivals)], second_recv
    ).wait()
    for o in range(devices):
        x_all[o * CAP : (o + 1) * CAP, :] = x_in[o]

    for k in range(1, ranks):
        peer = lax.rem(d + k, ranks)
        for i, (src, dst) in enumerate(((send_state, got_state), (send_cache, got_cache))):
            pltpu.make_async_remote_copy(
                src.at[peer], dst.at[d], mig_send.at[i], mig_recv.at[i],
                device_id=(peer, e), device_id_type=MESH,
            ).start()

    @pl.loop(0, up_tiles)
    def _(j):
        slot = lax.rem(j, ring)
        for copy in up_copies(j, slot):
            copy.wait()
        gate = jnp.dot(x_all[...], g_buf[slot], preferred_element_type=jnp.float32)
        upper = jnp.dot(x_all[...], u_buf[slot], preferred_element_type=jnp.float32)
        value = gate / (1.0 + jnp.exp(-gate)) * upper
        hidden[:, pl.ds(pl.multiple_of(j * UP_TILE, UP_TILE), UP_TILE)] = value.astype(jnp.bfloat16)

        @pl.when(j < up_tiles - ring)
        def _():
            for copy in up_copies(j + ring, slot):
                copy.start()

    @pl.loop(0, down_tiles)
    def _(c):
        down_copy(c).wait()
        part = jnp.dot(hidden[...], d_buf[c], preferred_element_type=jnp.float32)
        for o in range(devices):
            send_buf[c, o] = part[o * CAP : (o + 1) * CAP].astype(jnp.bfloat16)
        recv_buf[c, me] = send_buf[c, me]

        @pl.loop(1, devices)
        def _(k):
            other = lax.rem(me + k, devices)
            pltpu.make_async_remote_copy(
                send_buf.at[c, other], recv_buf.at[c, me], back_send.at[c], back_recv.at[c],
                device_id=(other // quads, lax.rem(other, quads)), device_id_type=MESH,
            ).start()

    @pl.loop(0, down_tiles)
    def _(c):
        most = recv_buf.at[c, pl.ds(0, devices - 1)]
        pltpu.make_async_copy(most, most, back_recv.at[c]).wait()
        rows_in = jnp.concatenate([recv_buf[c, o] for o in range(devices)], axis=0)
        high = jnp.dot(comb_high, rows_in, preferred_element_type=jnp.float32)
        low = jnp.dot(comb_low, rows_in, preferred_element_type=jnp.float32)
        mixed_ref[:, pl.ds(pl.multiple_of(c * DOWN_TILE, DOWN_TILE), DOWN_TILE)] = (
            high + low
        ).astype(jnp.bfloat16)

    for i, dst in enumerate((got_state, got_cache)):
        most = dst.at[pl.ds(0, ranks - 1)]
        pltpu.make_async_copy(most, most, mig_recv.at[i]).wait()
        pltpu.make_async_copy(most, most, mig_send.at[i]).wait()
    most = x_in.at[pl.ds(0, ranks - 1)]
    pltpu.make_async_copy(most, most, first_send).wait()
    most = x_in.at[pl.ds(0, arrivals)]
    pltpu.make_async_copy(most, most, second_send).wait()

    @pl.loop(0, down_tiles)
    def _(c):
        most = send_buf.at[c, pl.ds(0, devices - 1)]
        pltpu.make_async_copy(most, most, back_send.at[c]).wait()


def fused(
    tokens, router, expert_ids, w_gate, w_up, w_down, states, kv_blocks,
    plan_slots, plan_len, plan_blocks,
):
    ranks, quads = lax.axis_size("dp"), lax.axis_size("ep")
    devices = ranks * quads
    experts = router.shape[1]
    tok_count, width = tokens.shape
    moves = plan_slots.shape[1]
    per_request = plan_blocks.shape[3]
    bf16 = jnp.bfloat16
    dma = pltpu.SemaphoreType.DMA
    like = jax.ShapeDtypeStruct
    state_one, cache_one = states.shape[1:], kv_blocks.shape[1:]
    ids = expert_ids.T
    slots = jnp.transpose(plan_slots, (2, 1, 0))
    lengths = plan_len.T
    blocks = jnp.transpose(plan_blocks, (1, 2, 3, 0))
    depth = w_gate.shape[2]
    ring = min(RING, depth // UP_TILE)
    down_tiles = width // DOWN_TILE
    mixed, got_state, got_cache = pl.pallas_call(
        functools.partial(expert_kernel, ranks, quads),
        out_shape=(
            like((tok_count, width), bf16),
            like((ranks, *state_one), bf16),
            like((ranks, per_request, *cache_one), bf16),
        ),
        in_specs=[SMEM] * 4 + [VMEM] * 2 + [ANY] * 5,
        out_specs=(VMEM, ANY, ANY),
        scratch_shapes=[
            pltpu.VMEM((experts, CAP, width), bf16),
            pltpu.VMEM(states.shape, bf16),
            pltpu.VMEM(kv_blocks.shape, bf16),
            pltpu.VMEM((moves, *state_one), bf16),
            pltpu.VMEM((moves, per_request, *cache_one), bf16),
            pltpu.VMEM((ranks, *state_one), bf16),
            pltpu.VMEM((ranks, per_request, *cache_one), bf16),
            dma((2,)),
            pltpu.VMEM((ring, width, UP_TILE), bf16),
            pltpu.VMEM((ring, width, UP_TILE), bf16),
            pltpu.VMEM((down_tiles, depth, DOWN_TILE), bf16),
            pltpu.VMEM((devices, CAP, width), bf16),
            pltpu.VMEM((devices * CAP, width), bf16),
            pltpu.VMEM((devices * CAP, depth), bf16),
            pltpu.VMEM((down_tiles, devices, CAP, DOWN_TILE), bf16),
            pltpu.VMEM((down_tiles, devices, CAP, DOWN_TILE), bf16),
            dma((ring,)), dma((ring,)), dma((down_tiles,)), dma,
            dma, dma((ranks,)), dma, dma,
            dma((down_tiles,)), dma((down_tiles,)), dma((2,)), dma((2,)),
        ],
        compiler_params=pltpu.CompilerParams(
            collective_id=0, has_side_effects=True, vmem_limit_bytes=VMEM_LIMIT
        ),
        name="expert",
    )(
        ids, slots, lengths, blocks, tokens, router.T, w_gate, w_up, w_down, states, kv_blocks
    )
    new_states, new_cache, mixed = pl.pallas_call(
        land_kernel,
        out_shape=(like(states.shape, bf16), like(kv_blocks.shape, bf16), like(mixed.shape, bf16)),
        in_specs=[SMEM, SMEM] + [ANY] * 5,
        out_specs=(ANY, ANY, ANY),
        scratch_shapes=[
            pltpu.VMEM(states.shape, bf16),
            pltpu.VMEM(kv_blocks.shape, bf16),
            pltpu.VMEM(mixed.shape, bf16),
            pltpu.VMEM((moves, *state_one), bf16),
            pltpu.VMEM((moves, per_request, *cache_one), bf16),
            dma((3,)), dma((moves,)), dma((moves, per_request)), dma((3,)),
        ],
        name="land",
    )(slots, blocks, got_state, got_cache, states, kv_blocks, mixed)
    return mixed, new_states, new_cache


def local(
    tokens,
    router,
    expert_ids,
    w_gate,
    w_up,
    w_down,
    states,
    kv_blocks,
    plan_slots,
    plan_len,
    plan_blocks,
):
    ranks = lax.axis_size("dp")
    here = lax.axis_index("dp")
    moves = plan_slots.shape[1]
    slot_count = states.shape[0]
    block_count = kv_blocks.shape[0]
    per_request = plan_blocks.shape[3]
    block_len = kv_blocks.shape[2]
    mine = lax.dynamic_index_in_dim(plan_slots, here, 0, keepdims=False)
    my_blocks = lax.dynamic_index_in_dim(plan_blocks, here, 0, keepdims=False)
    my_length = lax.dynamic_index_in_dim(plan_len, here, 0, keepdims=False)
    leaving_slot = mine[:, 0]
    leaving_block = my_blocks[:, 0, :]
    state_out = states[jnp.maximum(leaving_slot, 0)]
    state_out = jnp.where((leaving_slot >= 0)[:, None, None], state_out, jnp.zeros_like(state_out))
    cache_out = kv_blocks[jnp.maximum(leaving_block, 0)]
    position = jnp.arange(per_request)[:, None] * block_len + jnp.arange(block_len)[None, :]
    written = (leaving_block >= 0)[:, :, None] & (position[None] < my_length[:, None, None])
    cache_out = jnp.where(written[:, :, None, :, None], cache_out, jnp.zeros_like(cache_out))
    arrivals = plan_slots[:, :, 1] == here
    sender = jnp.sum(jnp.where(arrivals, jnp.arange(ranks)[:, None], 0), axis=0)
    arriving = jnp.any(arrivals, axis=0)
    peers = jnp.arange(ranks)
    match = mine[:, 1][None, :] == peers[:, None]
    which = jnp.sum(jnp.where(match, jnp.arange(moves)[None, :], 0), axis=1)
    filled = jnp.any(match, axis=1)
    send_state = jnp.where(
        filled[:, None, None], state_out[which], jnp.zeros_like(state_out[which])
    )
    send_cache = jnp.where(
        filled[:, None, None, None, None], cache_out[which], jnp.zeros_like(cache_out[which])
    )
    got_state, got_cache = (
        lax.all_to_all(send_state, "dp", split_axis=0, concat_axis=0, tiled=True),
        lax.all_to_all(send_cache, "dp", split_axis=0, concat_axis=0, tiled=True),
    )
    state_in = got_state[sender]
    cache_in = got_cache[sender]
    slot_line = jnp.arange(slot_count)
    gone = jnp.any(slot_line[:, None] == leaving_slot[None, :], axis=1)
    new_states = jnp.where(gone[:, None, None], jnp.zeros_like(states), states)
    block_line = jnp.arange(block_count)
    gone_blocks = jnp.any(block_line[:, None, None] == leaving_block[None], axis=(1, 2))
    new_cache = jnp.where(gone_blocks[:, None, None, None], jnp.zeros_like(kv_blocks), kv_blocks)
    for move_index in range(moves):
        anchor = sender[move_index]
        place = plan_slots[anchor, move_index, 2]
        landing = (slot_line == place) & arriving[move_index]
        new_states = jnp.where(landing[:, None, None], state_in[move_index][None], new_states)
        for block_index in range(per_request):
            spot = plan_blocks[anchor, move_index, 1, block_index]
            block_hit = (block_line == spot) & arriving[move_index]
            new_cache = jnp.where(
                block_hit[:, None, None, None], cache_in[move_index, block_index][None], new_cache
            )
    experts = router.shape[1]
    tok_count = tokens.shape[0]
    width = tokens.shape[1]
    group = ranks // experts
    flat_ids = expert_ids.reshape(-1)
    onehot = (flat_ids[:, None] == jnp.arange(experts)[None, :]).astype(jnp.int32)
    earlier = jnp.cumsum(onehot, axis=0) - onehot
    slot_of = jnp.sum(earlier * onehot, axis=1)
    target_row = flat_ids * CAP + slot_of
    placer = (jnp.arange(experts * CAP)[:, None] == target_row[None, :]).astype(jnp.bfloat16)
    doubled = jnp.repeat(tokens, 2, axis=0)
    packed = jnp.dot(placer, doubled, preferred_element_type=jnp.float32).astype(jnp.bfloat16)
    outgoing = jnp.repeat(packed.reshape(experts, CAP, width), group, axis=0)
    incoming = lax.all_to_all(outgoing, "dp", split_axis=0, concat_axis=0, tiled=True)
    rows_in = incoming.reshape(ranks * CAP, width)
    piece = lax.all_gather(rows_in, "ep", axis=0, tiled=True)
    gate = jnp.dot(piece, w_gate[0], preferred_element_type=jnp.float32)
    upper = jnp.dot(piece, w_up[0], preferred_element_type=jnp.float32)
    hidden = (jax.nn.silu(gate) * upper).astype(jnp.bfloat16)
    summed = lax.psum_scatter(
        jnp.dot(hidden, w_down[0], preferred_element_type=jnp.float32),
        "ep",
        scatter_dimension=0,
        tiled=True,
    )
    returned = lax.all_to_all(
        summed.reshape(ranks, CAP, width), "dp", split_axis=0, concat_axis=0, tiled=True
    )
    expert_out = jnp.sum(returned.reshape(experts, group, CAP, width), axis=1).reshape(
        experts * CAP, width
    )
    chosen = expert_out[target_row].reshape(tok_count, 2, width)
    logits = jnp.dot(tokens.astype(jnp.float32), router, precision=lax.Precision.HIGHEST)
    scores = jax.nn.sigmoid(jnp.take_along_axis(logits, expert_ids, axis=1))
    weights = scores / jnp.sum(scores, axis=1, keepdims=True)
    mixed = jnp.sum(weights[:, :, None] * chosen, axis=1).astype(jnp.bfloat16)
    return (mixed, new_states, new_cache)


def solution(mesh):
    placed = (
        P(("dp", "ep"), None),
        P(),
        P(("dp", "ep"), None),
        P("dp", None, "ep"),
        P("dp", None, "ep"),
        P("dp", "ep", None),
        P("dp", None, "ep"),
        P("dp", None, None, "ep"),
        P(),
        P(),
        P(),
    )
    def step(*args):
        one_slab = args[1].shape[1] == lax.axis_size("dp")
        return (fused if one_slab else local)(*args)

    return jax.shard_map(
        step,
        mesh=mesh,
        in_specs=placed,
        out_specs=(P(("dp", "ep"), None), P("dp", None, "ep"), P("dp", None, None, "ep")),
        check_vma=False,
    )
```
